32 devices in a mesh: dp: 2 (over x), t: 4 (over z), stage: 4 (over y, core).
Axes of the slice: x: 2, y: 2, z: 4, core: 2. Of those that a mesh axis runs over, the one named last changes fastest.
Arguments:
- hidden: bfloat16 [8, 4, 128, 7168], P(('dp', 'stage')), parts along dimension 0
- w_query: bfloat16 [7168, 24576], P(None, 't')
- w_dkv: bfloat16 [7168, 576], replicated
- latent_gain: bfloat16 [512], replicated
- w_uk: bfloat16 [512, 16384], P(None, 't')
- w_uv: bfloat16 [512, 16384], P(None, 't')
- w_out: bfloat16 [16384, 7168], P('t')
Outputs:
- output 1: bfloat16 [8, 4, 128, 7168], P(('dp', 'stage')), parts along dimension 0
- output 2: bfloat16 [8, 4, 128, 576], P(('dp', 'stage'), 't'), parts along dimension 0
There are 2 independent parts. The reference program is written for one: setup_inputs(seed, part) draws one part's arguments, and reference() takes and returns one part's arrays. A program takes and returns all parts, laid end to end along the dimension named above; an argument that names none is the same for every part.
All inputs are finite; a program needn't handle non-finite values.
Results may differ from the reference program's by a relative error of at most 0.010829.
Values are sent between devices in bfloat16 or wider.
A program may use at most 1 GiB of HBM per device.

```python
import jax
import jax.numpy as jnp
from jax import lax

D_MODEL = 7168
HEADS = 128
KV_RANK = 512
ROPE_DIM = 64
NOPE_DIM = 128
V_DIM = 128
STAGE_SLOTS = 4
REQUESTS = 4
SEQ_LEN = 128

NORM_EPS = 1e-6
ROPE_BASE = 10000.0
HALF_ROPE = ROPE_DIM // 2
HEAD_DIM = NOPE_DIM + ROPE_DIM
PROMPT_SLOTS = STAGE_SLOTS // 2
N_BLOCKS = max(1, min(8, SEQ_LEN // 128))
BLOCK_LEN = SEQ_LEN // N_BLOCKS


def setup_inputs(seed: int = 0, part: int = 0) -> dict:
    part_key = jax.random.fold_in(jax.random.key(seed), part)
    shared = jax.random.split(jax.random.key(seed + 1), 6)
    hidden = jax.random.normal(part_key, (STAGE_SLOTS, REQUESTS, SEQ_LEN, D_MODEL), jnp.float32).astype(jnp.bfloat16)
    w_query = (jax.random.normal(shared[0], (D_MODEL, HEADS * HEAD_DIM), jnp.float32) * D_MODEL ** -0.5).astype(jnp.bfloat16)
    w_dkv = (jax.random.normal(shared[1], (D_MODEL, KV_RANK + ROPE_DIM), jnp.float32) * D_MODEL ** -0.5).astype(jnp.bfloat16)
    latent_gain = (1.0 + 0.3 * jax.random.normal(shared[2], (KV_RANK,), jnp.float32)).astype(jnp.bfloat16)
    w_uk = (jax.random.normal(shared[3], (KV_RANK, HEADS * NOPE_DIM), jnp.float32) * KV_RANK ** -0.5).astype(jnp.bfloat16)
    w_uv = (jax.random.normal(shared[4], (KV_RANK, HEADS * V_DIM), jnp.float32) * KV_RANK ** -0.5).astype(jnp.bfloat16)
    w_out = (jax.random.normal(shared[5], (HEADS * V_DIM, D_MODEL), jnp.float32) * (HEADS * V_DIM) ** -0.5).astype(jnp.bfloat16)
    return {"hidden": hidden, "w_query": w_query, "w_dkv": w_dkv, "latent_gain": latent_gain, "w_uk": w_uk, "w_uv": w_uv, "w_out": w_out}


def rope_tables():
    positions = jnp.arange(SEQ_LEN).astype(jnp.float32)
    inv_freq = ROPE_BASE ** (-jnp.arange(HALF_ROPE).astype(jnp.float32) / HALF_ROPE)
    angles = positions[:, None] * inv_freq[None, :]
    return jnp.cos(angles), jnp.sin(angles)


def apply_rope(vecs, cos_tab, sin_tab):
    as_f32 = vecs.astype(jnp.float32)
    low_half = as_f32[..., :HALF_ROPE]
    high_half = as_f32[..., HALF_ROPE:]
    rotated = jnp.concatenate([low_half * cos_tab - high_half * sin_tab, high_half * cos_tab + low_half * sin_tab], axis=-1)
    return rotated.astype(jnp.bfloat16)


def reference(hidden, w_query, w_dkv, latent_gain, w_uk, w_uv, w_out):
    cos_tab, sin_tab = rope_tables()

    def one_request(tokens):
        compressed = jnp.dot(tokens, w_dkv, preferred_element_type=jnp.float32).astype(jnp.bfloat16)
        c_raw = compressed[:, :KV_RANK].astype(jnp.float32)
        inv_rms = lax.rsqrt(jnp.mean(c_raw * c_raw, axis=-1, keepdims=True) + NORM_EPS)
        c_kv = (c_raw * inv_rms * latent_gain.astype(jnp.float32)).astype(jnp.bfloat16)
        k_rope = apply_rope(compressed[:, KV_RANK:], cos_tab, sin_tab)
        queries = jnp.dot(tokens, w_query, preferred_element_type=jnp.float32).astype(jnp.bfloat16)
        queries = queries.reshape(SEQ_LEN, HEADS, HEAD_DIM)
        q_nope = queries[:, :, :NOPE_DIM].astype(jnp.float32)
        q_rope = apply_rope(queries[:, :, NOPE_DIM:], cos_tab[:, None, :], sin_tab[:, None, :]).astype(jnp.float32)
        k_nope = jnp.dot(c_kv, w_uk, preferred_element_type=jnp.float32).astype(jnp.bfloat16)
        k_nope = k_nope.reshape(SEQ_LEN, HEADS, NOPE_DIM).astype(jnp.float32)
        values = jnp.dot(c_kv, w_uv, preferred_element_type=jnp.float32).astype(jnp.bfloat16)
        values = values.reshape(SEQ_LEN, HEADS, V_DIM).astype(jnp.float32)
        k_rope_f = k_rope.astype(jnp.float32)
        pieces = []
        for block_idx in range(N_BLOCKS):
            start_row = block_idx * BLOCK_LEN
            stop_row = start_row + BLOCK_LEN
            scores = jnp.einsum("qhe,khe->hqk", q_nope[start_row:stop_row], k_nope[:stop_row])
            scores = scores + jnp.einsum("qhe,ke->hqk", q_rope[start_row:stop_row], k_rope_f[:stop_row])
            q_pos = start_row + jnp.arange(BLOCK_LEN)[:, None]
            k_pos = jnp.arange(stop_row)[None, :]
            scores = jnp.where(k_pos <= q_pos, scores * HEAD_DIM ** -0.5, -jnp.inf)
            row_peak = jnp.max(scores, axis=-1, keepdims=True)
            weights = jnp.exp(scores - row_peak)
            row_total = jnp.sum(weights, axis=-1)
            mixed = jnp.einsum("hqk,khe->qhe", weights.astype(jnp.bfloat16).astype(jnp.float32), values[:stop_row])
            pieces.append((mixed / row_total.T[:, :, None]).astype(jnp.bfloat16))
        head_mix = jnp.concatenate(pieces, axis=0).reshape(SEQ_LEN, HEADS * V_DIM)
        out_rows = jnp.dot(head_mix, w_out, preferred_element_type=jnp.float32).astype(jnp.bfloat16)
        latent = jnp.concatenate([c_kv, k_rope], axis=-1)
        return out_rows, latent

    prompts = hidden[:PROMPT_SLOTS].reshape(PROMPT_SLOTS * REQUESTS, SEQ_LEN, D_MODEL)
    out_rows, latent = lax.map(one_request, prompts)
    out_rows = out_rows.reshape(PROMPT_SLOTS, REQUESTS, SEQ_LEN, D_MODEL)
    latent = latent.reshape(PROMPT_SLOTS, REQUESTS, SEQ_LEN, KV_RANK + ROPE_DIM)
    attn_out = jnp.concatenate([out_rows, jnp.zeros_like(out_rows)], axis=0)
    latent_cache = jnp.concatenate([jnp.zeros_like(latent), latent], axis=0)
    return attn_out, latent_cache
```

```python
import functools

import jax
import jax.numpy as jnp
from jax import lax
from jax.experimental import pallas as pl
from jax.experimental.pallas import tpu as pltpu
from jax.sharding import PartitionSpec as P

NOPE_DIM = 128
ROPE_DIM = 64
V_DIM = 128
NORM_EPS = 1e-6
ROPE_BASE = 10000.0
MESH = pl.DeviceIdType.MESH
TILE = 256
HOP_LAG = 2


def rope_tables(seq_len):
    half_dim = ROPE_DIM // 2
    positions = jnp.arange(seq_len, dtype=jnp.float32)
    inv_freq = ROPE_BASE ** (-jnp.arange(half_dim, dtype=jnp.float32) / half_dim)
    angles = positions[:, None] * inv_freq[None, :]
    return jnp.cos(angles), jnp.sin(angles)


def apply_rope(vecs, cos_tab, sin_tab):
    half_dim = vecs.shape[-1] // 2
    as_f32 = vecs.astype(jnp.float32)
    low_half = as_f32[..., :half_dim]
    high_half = as_f32[..., half_dim:]
    rotated = jnp.concatenate([low_half * cos_tab - high_half * sin_tab, high_half * cos_tab + low_half * sin_tab], axis=-1)
    return rotated.astype(jnp.bfloat16)


def latent_rows(tokens, w_dkv, latent_gain, cos_tab, sin_tab):
    kv_rank = latent_gain.shape[0]
    compressed = jnp.einsum("bsd,dc->bsc", tokens, w_dkv, preferred_element_type=jnp.float32).astype(jnp.bfloat16)
    c_raw = compressed[..., :kv_rank].astype(jnp.float32)
    inv_rms = lax.rsqrt(jnp.mean(c_raw * c_raw, axis=-1, keepdims=True) + NORM_EPS)
    c_kv = (c_raw * inv_rms * latent_gain.astype(jnp.float32)).astype(jnp.bfloat16)
    k_rope = apply_rope(compressed[..., kv_rank:], cos_tab, sin_tab)
    return jnp.concatenate([c_kv, k_rope], axis=-1)


def causal_heads(q_nope, q_rope, k_nope, k_rope, values):
    seq_len = q_nope.shape[1]
    n_blocks = max(1, min(8, seq_len // 128))
    block_len = seq_len // n_blocks
    score_scale = (q_nope.shape[-1] + q_rope.shape[-1]) ** -0.5
    pieces = []
    for block_idx in range(n_blocks):
        start_row = block_idx * block_len
        stop_row = start_row + block_len
        scores = jnp.einsum("bqhe,bkhe->bhqk", q_nope[:, start_row:stop_row], k_nope[:, :stop_row], preferred_element_type=jnp.float32)
        scores = scores + jnp.einsum("bqhe,bke->bhqk", q_rope[:, start_row:stop_row], k_rope[:, :stop_row], preferred_element_type=jnp.float32)
        q_pos = start_row + jnp.arange(block_len)[:, None]
        k_pos = jnp.arange(stop_row)[None, :]
        scores = jnp.where(k_pos <= q_pos, scores * score_scale, -jnp.inf)
        row_peak = jnp.max(scores, axis=-1, keepdims=True)
        weights = jnp.exp(scores - row_peak)
        row_total = jnp.sum(weights, axis=-1)
        mixed = jnp.einsum("bhqk,bkhe->bqhe", weights.astype(jnp.bfloat16), values[:, :stop_row], preferred_element_type=jnp.float32)
        pieces.append((mixed / jnp.transpose(row_total, (0, 2, 1))[..., None]).astype(jnp.bfloat16))
    return jnp.concatenate(pieces, axis=1)


def head_outputs(tokens, latent, w_query, w_uk, w_uv, cos_tab, sin_tab):
    kv_rank = w_uk.shape[0]
    batch, seq_len = tokens.shape[0], tokens.shape[1]
    heads_here = w_uk.shape[1] // NOPE_DIM
    queries = jnp.einsum("bsd,dn->bsn", tokens, w_query, preferred_element_type=jnp.float32).astype(jnp.bfloat16)
    queries = queries.reshape(batch, seq_len, heads_here, NOPE_DIM + ROPE_DIM)
    q_rope = apply_rope(queries[..., NOPE_DIM:], cos_tab[:, None, :], sin_tab[:, None, :])
    k_nope = jnp.einsum("bsr,rn->bsn", latent[..., :kv_rank], w_uk, preferred_element_type=jnp.float32).astype(jnp.bfloat16)
    k_nope = k_nope.reshape(batch, seq_len, heads_here, NOPE_DIM)
    values = jnp.einsum("bsr,rn->bsn", latent[..., :kv_rank], w_uv, preferred_element_type=jnp.float32).astype(jnp.bfloat16)
    values = values.reshape(batch, seq_len, heads_here, V_DIM)
    head_mix = causal_heads(queries[..., :NOPE_DIM], q_rope, k_nope, latent[..., kv_rank:], values)
    return head_mix.reshape(batch * seq_len, heads_here * V_DIM)


def project_reduce_kernel(n_tiles, n_steps, o_ref, w_ref, lat_ref, out_ref, cache_ref, part, partb, ebuf, ibuf,
                          send_b, recv_p, send_e, recv_e, send_i, recv_i, send_f, send_o, recv_o, local_sem, lat_sem):
    step = pl.program_id(0)
    t = lax.axis_index("t")
    stage = lax.axis_index("stage")
    is_prompt = stage < 2
    is_relay = stage >= 2
    partner = lax.rem(stage + 2, 4)
    is_end = (t == 0) | (t == 3)
    is_inner = (t == 1) | (t == 2)
    peer = 3 - t
    inner_nb = jnp.where(t == 0, 1, 2)
    end_nb = jnp.where(t == 1, 0, 3)
    half = part.shape[1]
    seq = cache_ref.shape[0]

    def to_partner(j):
        return pltpu.make_async_remote_copy(src_ref=partb.at[j], dst_ref=part.at[j], send_sem=send_b.at[j], recv_sem=recv_p.at[j],
                                            device_id={"stage": partner}, device_id_type=MESH)

    def end_to_inner(j):
        return pltpu.make_async_remote_copy(src_ref=part.at[j], dst_ref=ebuf.at[j], send_sem=send_e.at[j], recv_sem=recv_e.at[j],
                                            device_id={"t": inner_nb}, device_id_type=MESH)

    def inner_to_peer(j):
        return pltpu.make_async_remote_copy(src_ref=part.at[j], dst_ref=ibuf.at[j], send_sem=send_i.at[j], recv_sem=recv_i.at[j],
                                            device_id={"t": peer}, device_id_type=MESH)

    def final_to_end(j, src):
        return pltpu.make_async_remote_copy(src_ref=src.at[j], dst_ref=ibuf.at[j], send_sem=send_f.at[j], recv_sem=recv_i.at[j],
                                            device_id={"t": end_nb}, device_id_type=MESH)

    def cols(j):
        return pl.ds(pl.multiple_of(j * TILE, TILE), TILE)

    def final_back(j, src):
        return pltpu.make_async_remote_copy(src_ref=src.at[j], dst_ref=out_ref.at[pl.ds(half, half), cols(j)], send_sem=send_o.at[j],
                                            recv_sem=recv_o.at[j], device_id={"stage": partner}, device_id_type=MESH)

    def final_local(j, src):
        return pltpu.make_async_copy(src.at[j], out_ref.at[pl.ds(0, half), cols(j)], local_sem.at[j])

    def cache_copy():
        return pltpu.make_async_remote_copy(src_ref=lat_ref.at[pl.ds(pl.multiple_of(t * seq, seq), seq)], dst_ref=cache_ref, send_sem=lat_sem.at[0],
                                            recv_sem=lat_sem.at[1], device_id={"stage": partner}, device_id_type=MESH)

    def deliver(j, src):
        @pl.when(is_prompt)
        def _():
            final_local(j, src).start()

        @pl.when(is_relay)
        def _():
            final_back(j, src).start()

    def live(j):
        return (j >= 0) & (j < n_tiles)

    @pl.when(step == 0)
    def _():
        barrier = pltpu.get_barrier_semaphore()
        pl.semaphore_signal(barrier, inc=1, device_id={"stage": partner}, device_id_type=MESH)

        @pl.when(is_end)
        def _():
            pl.semaphore_signal(barrier, inc=1, device_id={"t": inner_nb}, device_id_type=MESH)
            pl.semaphore_wait(barrier, 2)

        @pl.when(is_inner)
        def _():
            pl.semaphore_signal(barrier, inc=1, device_id={"t": end_nb}, device_id_type=MESH)
            pl.semaphore_signal(barrier, inc=1, device_id={"t": peer}, device_id_type=MESH)
            pl.semaphore_wait(barrier, 3)

        @pl.when(is_prompt)
        def _():
            cache_copy().start()

    @pl.when(is_prompt & (step < n_tiles))
    def _():
        full = jnp.dot(o_ref[...], w_ref[...], preferred_element_type=jnp.float32).astype(jnp.bfloat16)
        part[step] = full[:half]
        partb[step] = full[half:]
        to_partner(step).start()

    own = step - jnp.where(is_relay, HOP_LAG, 0)

    @pl.when(is_relay & live(own))
    def _():
        to_partner(own).wait_recv()

    @pl.when(is_end & live(own))
    def _():
        end_to_inner(own).start()

    first = own - HOP_LAG
    root_first = 1 + lax.rem(first + 2 * n_tiles, 2)

    @pl.when(is_inner & live(first))
    def _():
        end_to_inner(first).wait_recv()

        @pl.when(t != root_first)
        def _():
            part[first] = (part[first].astype(jnp.float32) + ebuf[first].astype(jnp.float32)).astype(jnp.bfloat16)
            inner_to_peer(first).start()

    second = first - HOP_LAG
    root_second = 1 + lax.rem(second + 2 * n_tiles, 2)

    @pl.when(is_inner & live(second) & (t == root_second))
    def _():
        inner_to_peer(second).wait_recv()
        total = part[second].astype(jnp.float32) + ebuf[second].astype(jnp.float32) + ibuf[second].astype(jnp.float32)
        part[second] = total.astype(jnp.bfloat16)
        inner_to_peer(second).start()
        final_to_end(second, part).start()
        deliver(second, part)

    third = second - HOP_LAG
    root_third = 1 + lax.rem(third + 2 * n_tiles, 2)

    @pl.when(is_inner & live(third) & (t != root_third))
    def _():
        inner_to_peer(third).wait_recv()
        final_to_end(third, ibuf).start()
        deliver(third, ibuf)

    fourth = third - HOP_LAG

    @pl.when(is_end & live(fourth))
    def _():
        final_to_end(fourth, ibuf).wait_recv()
        deliver(fourth, ibuf)

    @pl.when(step == n_steps - 1)
    def _():
        @pl.loop(0, n_tiles)
        def _(j):
            @pl.when(is_end)
            def _():
                end_to_inner(j).wait_send()

            @pl.when(is_inner)
            def _():
                inner_to_peer(j).wait_send()
                final_to_end(j, part).wait_send()

            @pl.when(is_prompt)
            def _():
                to_partner(j).wait_send()
                final_local(j, part).wait()
                final_back(j, part).wait_recv()

            @pl.when(is_relay)
            def _():
                final_back(j, part).wait_send()

        @pl.when(is_prompt)
        def _():
            cache_copy().wait_send()

        @pl.when(is_relay)
        def _():
            cache_copy().wait_recv()


def project_reduce(head_mix, w_out, latent, seq_len):
    rows, depth = head_mix.shape
    width = w_out.shape[1]
    n_tiles = width // TILE
    n_steps = n_tiles + 5 * HOP_LAG
    half = rows // 2
    any_spec = pl.BlockSpec(memory_space=pl.ANY)
    chunk = pltpu.VMEM((n_tiles, half, TILE), jnp.bfloat16)
    return pl.pallas_call(
        functools.partial(project_reduce_kernel, n_tiles, n_steps),
        grid=(n_steps,),
        out_shape=(jax.ShapeDtypeStruct((rows, width), jnp.bfloat16), jax.ShapeDtypeStruct((seq_len, latent.shape[1]), jnp.bfloat16)),
        in_specs=[
            pl.BlockSpec((rows, depth), lambda i: (0, 0)),
            pl.BlockSpec((depth, TILE), lambda i: (0, jnp.minimum(i, n_tiles - 1))),
            any_spec,
        ],
        out_specs=(any_spec, any_spec),
        scratch_shapes=[chunk, chunk, chunk, chunk] + [pltpu.SemaphoreType.DMA((n_tiles,))] * 10 + [pltpu.SemaphoreType.DMA((2,))],
        compiler_params=pltpu.CompilerParams(collective_id=0, has_side_effects=True, vmem_limit_bytes=56 * 1024 * 1024),
    )(head_mix, w_out, latent)


def solution(mesh):
    half_stage = mesh.shape["stage"] // 2
    slot_spec = P(("dp", "stage"), None, None, None)
    cache_spec = P(("dp", "stage"), "t", None, None)

    def device_step(hidden, w_query, w_dkv, latent_gain, w_uk, w_uv, w_out):
        tokens = hidden[0]
        batch, seq_len, width = tokens.shape
        cos_tab, sin_tab = rope_tables(seq_len)
        latent = latent_rows(tokens, w_dkv, latent_gain, cos_tab, sin_tab)
        head_mix = head_outputs(tokens, latent, w_query, w_uk, w_uv, cos_tab, sin_tab)
        summed, handed = project_reduce(head_mix, w_out, latent.reshape(batch * seq_len, -1), seq_len)
        is_prompt = lax.axis_index("stage") < half_stage
        out_rows = jnp.where(is_prompt, summed, jnp.zeros_like(summed)).reshape(batch, seq_len, width)
        cache = jnp.where(is_prompt, jnp.zeros_like(handed), handed)
        return out_rows[None], cache[None, None]

    return jax.shard_map(device_step, mesh=mesh, in_specs=(slot_spec, P(None, "t"), P(None, None), P(None), P(None, "t"), P(None, "t"), P("t", None)), out_specs=(slot_spec, cache_spec), check_vma=False)
```

```python
import functools

import jax
import jax.numpy as jnp
import numpy as np
from jax import lax
from jax.experimental import pallas as pl
from jax.experimental.pallas import tpu as pltpu
from jax.sharding import PartitionSpec as P

NOPE_DIM = 128
ROPE_DIM = 64
V_DIM = 128
NORM_EPS = 1e-6
ROPE_BASE = 10000.0
MESH = pl.DeviceIdType.MESH
TILE = 512
HOP_LAG = 2
HEADS_STEP = 4
PIECE = 16


def rope_tables(seq_len):
    half_dim = ROPE_DIM // 2
    positions = jnp.arange(seq_len, dtype=jnp.float32)
    inv_freq = ROPE_BASE ** (-jnp.arange(half_dim, dtype=jnp.float32) / half_dim)
    angles = positions[:, None] * inv_freq[None, :]
    return jnp.cos(angles), jnp.sin(angles)


def apply_rope(vecs, cos_tab, sin_tab):
    half_dim = vecs.shape[-1] // 2
    as_f32 = vecs.astype(jnp.float32)
    low_half = as_f32[..., :half_dim]
    high_half = as_f32[..., half_dim:]
    rotated = jnp.concatenate([low_half * cos_tab - high_half * sin_tab, high_half * cos_tab + low_half * sin_tab], axis=-1)
    return rotated.astype(jnp.bfloat16)


def latent_rows(tokens, w_dkv, latent_gain, cos_tab, sin_tab):
    kv_rank = latent_gain.shape[0]
    compressed = jnp.einsum("bsd,dc->bsc", tokens, w_dkv, preferred_element_type=jnp.float32).astype(jnp.bfloat16)
    c_raw = compressed[..., :kv_rank].astype(jnp.float32)
    inv_rms = lax.rsqrt(jnp.mean(c_raw * c_raw, axis=-1, keepdims=True) + NORM_EPS)
    c_kv = (c_raw * inv_rms * latent_gain.astype(jnp.float32)).astype(jnp.bfloat16)
    k_rope = apply_rope(compressed[..., kv_rank:], cos_tab, sin_tab)
    return jnp.concatenate([c_kv, k_rope], axis=-1)


def lane_tables(seq_len):
    half_dim = ROPE_DIM // 2
    inv_freq = np.float32(ROPE_BASE) ** (-np.arange(half_dim, dtype=np.float32) / np.float32(half_dim))
    angles = np.arange(seq_len, dtype=np.float32)[:, None] * inv_freq[None, :].astype(np.float32)
    cos_tab, sin_tab = np.cos(angles).astype(np.float32), np.sin(angles).astype(np.float32)
    one, zero = np.ones((seq_len, ROPE_DIM), np.float32), np.zeros((seq_len, ROPE_DIM), np.float32)
    cos_low = np.concatenate([cos_tab, cos_tab, one], axis=1)
    sin_low = np.concatenate([-sin_tab, sin_tab, zero], axis=1)
    cos_high = np.concatenate([one, cos_tab, cos_tab], axis=1)
    sin_high = np.concatenate([zero, -sin_tab, sin_tab], axis=1)
    return cos_low, sin_low, cos_high, sin_high


def rope_lanes(vecs, cos_tab, sin_tab, pick_up):
    as_f32 = vecs.astype(jnp.float32)
    turned = jnp.where(pick_up, pltpu.roll(as_f32, 96, 1), pltpu.roll(as_f32, 32, 1))
    return (as_f32 * cos_tab + turned * sin_tab).astype(jnp.bfloat16)


def project_heads(rows, slot, x_ref, wq_ref, wuk_ref, wuv_ref, lat_ref, q_buf, k_buf, v_buf):
    kv_rank = wuk_ref.shape[0]
    q_buf[slot, :rows] = jnp.dot(x_ref[:rows], wq_ref[...], preferred_element_type=jnp.float32).astype(jnp.bfloat16)
    c_kv = lat_ref[:rows, :kv_rank]
    k_buf[slot, :rows] = jnp.dot(c_kv, wuk_ref[...], preferred_element_type=jnp.float32).astype(jnp.bfloat16)
    v_buf[slot, :rows] = jnp.dot(c_kv, wuv_ref[...], preferred_element_type=jnp.float32).astype(jnp.bfloat16)


def attend_request(q_ref, k_ref, v_ref, lat_ref, tabs, here, seq):
    kv_rank = lat_ref.shape[1] - 128
    cos_low, sin_low, cos_high, sin_high = (tab[...] for tab in tabs)
    lane = lax.broadcasted_iota(jnp.int32, (seq, 128), 1)
    low = lane < 64
    pick_up = (lane & 32) == 0
    key_rope = lat_ref[here, kv_rank:]
    key_rope_high = pltpu.roll(key_rope.astype(jnp.float32), 64, 1)
    causal = lax.broadcasted_iota(jnp.int32, (seq, seq), 1) <= lax.broadcasted_iota(jnp.int32, (seq, seq), 0)
    scale = (NOPE_DIM + ROPE_DIM) ** -0.5
    all_scores = []
    for pair in range(HEADS_STEP // 2):
        base = 384 * pair
        q_a = q_ref[here, base:base + 128]
        q_b = rope_lanes(q_ref[here, base + 128:base + 256], cos_low, sin_low, pick_up)
        q_c = rope_lanes(q_ref[here, base + 256:base + 384], cos_high, sin_high, pick_up)
        k_even = k_ref[here, 256 * pair:256 * pair + 128]
        k_odd = pltpu.roll(k_ref[here, 256 * pair + 128:256 * pair + 256].astype(jnp.float32), 64, 1)
        k_odd_a = jnp.where(low, 0.0, k_odd).astype(jnp.bfloat16)
        k_odd_b = jnp.where(low, k_odd, key_rope_high).astype(jnp.bfloat16)
        sides = ((jnp.concatenate([q_a, q_b], axis=1), jnp.concatenate([k_even, key_rope], axis=1)),
                 (jnp.concatenate([q_b, q_c], axis=1), jnp.concatenate([k_odd_a, k_odd_b], axis=1)))
        for q_side, k_side in sides:
            all_scores.append(lax.dot_general(q_side, k_side, (((1,), (1,)), ((), ())), preferred_element_type=jnp.float32))
    mixes = []
    for head, scores in enumerate(all_scores):
        scores = jnp.where(causal, scores * scale, -jnp.inf)
        weights = jnp.exp(scores - jnp.max(scores, axis=1, keepdims=True))
        total = jnp.sum(weights, axis=1, keepdims=True)
        mixed = jnp.dot(weights.astype(jnp.bfloat16), v_ref[here, 128 * head:128 * head + 128], preferred_element_type=jnp.float32)
        mixes.append((mixed / total).astype(jnp.bfloat16))
    return jnp.concatenate(mixes, axis=1)


def prefill_kernel(n_heads_steps, n_tiles, x_src, wq_ref, wuk_ref, wuv_ref, lat_src, tab_a, tab_b, tab_c, tab_d, w_ref, cache_src,
                   out_ref, cache_ref, x_ref, lat_ref, q_buf, k_buf, v_buf, heads_out, part, partb, ebuf, ibuf,
                   send_x, recv_x, send_n, recv_n, send_b, recv_p, send_e, recv_e, send_i, recv_i, send_f, send_o, recv_o, local_sem, lat_sem, load_sem):
    step = pl.program_id(0)
    n_chunks = 2 * n_tiles
    t = lax.axis_index("t")
    stage = lax.axis_index("stage")
    is_prompt = stage < 2
    is_relay = stage >= 2
    partner = lax.rem(stage + 2, 4)
    is_end = (t == 0) | (t == 3)
    is_inner = (t == 1) | (t == 2)
    peer = 3 - t
    inner_nb = jnp.where(t == 0, 1, 2)
    end_nb = jnp.where(t == 1, 0, 3)
    pair_nb = jnp.where(is_end, inner_nb, end_nb)
    seq = cache_ref.shape[0]
    prompt_rows = x_ref.shape[0]
    half = seq // 2
    side = lax.rem(t, 2)
    n_pieces = half // PIECE
    drain = step == n_heads_steps + n_tiles
    in_heads = step < n_heads_steps
    in_tiles = (step >= n_heads_steps) & (step < n_heads_steps + n_tiles)

    def tokens_over(p):
        src = pl.multiple_of(prompt_rows + side * half + p * PIECE, PIECE)
        dst = pl.multiple_of(side * half + p * PIECE, PIECE)
        return pltpu.make_async_remote_copy(src_ref=x_src.at[pl.ds(src, PIECE)], dst_ref=x_ref.at[pl.ds(dst, PIECE)], send_sem=send_x.at[p],
                                            recv_sem=recv_x.at[p], device_id={"stage": partner}, device_id_type=MESH)

    def latent_over():
        src = pl.multiple_of(prompt_rows + side * half, half)
        dst = pl.multiple_of(side * half, half)
        return pltpu.make_async_remote_copy(src_ref=lat_src.at[pl.ds(src, half)], dst_ref=lat_ref.at[pl.ds(dst, half)], send_sem=send_x.at[n_pieces],
                                            recv_sem=recv_x.at[n_pieces], device_id={"stage": partner}, device_id_type=MESH)

    def tokens_next(p, which):
        rows = pl.ds(pl.multiple_of(which * half + p * PIECE, PIECE), PIECE)
        return pltpu.make_async_remote_copy(src_ref=x_ref.at[rows], dst_ref=x_ref.at[rows], send_sem=send_n.at[p],
                                            recv_sem=recv_n.at[p], device_id={"t": pair_nb}, device_id_type=MESH)

    def latent_next(which):
        rows = pl.ds(pl.multiple_of(which * half, half), half)
        return pltpu.make_async_remote_copy(src_ref=lat_ref.at[rows], dst_ref=lat_ref.at[rows], send_sem=send_n.at[n_pieces],
                                            recv_sem=recv_n.at[n_pieces], device_id={"t": pair_nb}, device_id_type=MESH)

    def to_partner(tile):
        return pltpu.make_async_remote_copy(src_ref=partb.at[tile], dst_ref=part.at[2 * tile], send_sem=send_b.at[tile], recv_sem=recv_p.at[tile],
                                            device_id={"stage": partner}, device_id_type=MESH)

    def end_to_inner(c):
        return pltpu.make_async_remote_copy(src_ref=part.at[c], dst_ref=ebuf.at[c], send_sem=send_e.at[c], recv_sem=recv_e.at[c],
                                            device_id={"t": inner_nb}, device_id_type=MESH)

    def inner_to_peer(c):
        return pltpu.make_async_remote_copy(src_ref=part.at[c], dst_ref=ibuf.at[c], send_sem=send_i.at[c], recv_sem=recv_i.at[c],
                                            device_id={"t": peer}, device_id_type=MESH)

    def final_to_end(c, src):
        return pltpu.make_async_remote_copy(src_ref=src.at[c], dst_ref=ibuf.at[c], send_sem=send_f.at[c], recv_sem=recv_i.at[c],
                                            device_id={"t": end_nb}, device_id_type=MESH)

    def place(c, line):
        row = (2 * line + lax.rem(c, 2)) * seq
        col = lax.div(c, 2) * TILE
        return out_ref.at[pl.ds(pl.multiple_of(row, seq), seq), pl.ds(pl.multiple_of(col, TILE), TILE)]

    def final_back(c, src):
        return pltpu.make_async_remote_copy(src_ref=src.at[c], dst_ref=place(c, 1), send_sem=send_o.at[c],
                                            recv_sem=recv_o.at[c], device_id={"stage": partner}, device_id_type=MESH)

    def final_local(c, src):
        return pltpu.make_async_copy(src.at[c], place(c, 0), local_sem.at[c])

    def cache_copy():
        return pltpu.make_async_remote_copy(src_ref=cache_src.at[pl.ds(pl.multiple_of(t * seq, seq), seq)], dst_ref=cache_ref, send_sem=lat_sem.at[0],
                                            recv_sem=lat_sem.at[1], device_id={"stage": partner}, device_id_type=MESH)

    def deliver(c, src):
        @pl.when(is_prompt)
        def _():
            final_local(c, src).start()

        @pl.when(is_relay)
        def _():
            final_back(c, src).start()

    @pl.when(step == 0)
    def _():
        barrier = pltpu.get_barrier_semaphore()
        pl.semaphore_signal(barrier, inc=1, device_id={"stage": partner}, device_id_type=MESH)

        @pl.when(is_end)
        def _():
            pl.semaphore_signal(barrier, inc=1, device_id={"t": inner_nb}, device_id_type=MESH)
            pl.semaphore_wait(barrier, 2)

        @pl.when(is_inner)
        def _():
            pl.semaphore_signal(barrier, inc=1, device_id={"t": end_nb}, device_id_type=MESH)
            pl.semaphore_signal(barrier, inc=1, device_id={"t": peer}, device_id_type=MESH)
            pl.semaphore_wait(barrier, 3)

        @pl.when(is_prompt)
        def _():
            load_x = pltpu.make_async_copy(x_src.at[pl.ds(0, prompt_rows)], x_ref, load_sem.at[0])
            load_lat = pltpu.make_async_copy(lat_src.at[pl.ds(0, prompt_rows)], lat_ref, load_sem.at[1])
            load_x.start()
            load_lat.start()

            @pl.loop(0, n_pieces)
            def _(p):
                tokens_over(p).start()

            latent_over().start()
            load_x.wait()
            load_lat.wait()

        @pl.when(is_relay)
        def _():
            @pl.loop(0, n_pieces)
            def _(p):
                tokens_over(p).wait_recv()
                tokens_next(p, side).start()

            latent_over().wait_recv()
            latent_next(side).start()

            @pl.loop(0, n_pieces)
            def _(p):
                tokens_next(p, 1 - side).wait_recv()

            latent_next(1 - side).wait_recv()

    def attend(rows):
        width = HEADS_STEP * V_DIM
        slot = lax.rem(step + 1, 2)
        done = lax.rem(step + n_heads_steps - 1, n_heads_steps)
        for req in range(rows // seq):
            here = slice(req * seq, (req + 1) * seq)
            heads_out[here, pl.ds(pl.multiple_of(done * width, width), width)] = attend_request(
                q_buf.at[slot], k_buf.at[slot], v_buf.at[slot], lat_ref, (tab_a, tab_b, tab_c, tab_d), here, seq)

    for mine, rows in ((is_prompt, prompt_rows), (is_relay, seq)):
        @pl.when(mine & in_heads)
        def _():
            attend(rows)
            project_heads(rows, lax.rem(step, 2), x_ref, wq_ref, wuk_ref, wuv_ref, lat_ref, q_buf, k_buf, v_buf)

        @pl.when(mine & (step == n_heads_steps))
        def _():
            attend(rows)

    @pl.when(is_prompt & (step == n_heads_steps))
    def _():
        cache_copy().start()

    @pl.when(is_prompt & in_tiles)
    def _():
        tile = step - n_heads_steps
        full = jnp.dot(heads_out[...], w_ref[...], preferred_element_type=jnp.float32).astype(jnp.bfloat16)
        part[2 * tile] = full[:seq]
        part[2 * tile + 1] = full[seq:2 * seq]
        partb[tile] = full[2 * seq:]
        to_partner(tile).start()

        @pl.when(is_end)
        def _():
            end_to_inner(2 * tile).start()
            end_to_inner(2 * tile + 1).start()

    @pl.when(is_relay & in_tiles)
    def _():
        c = 2 * (step - n_heads_steps) + 1
        part[c] = jnp.dot(heads_out[:seq], w_ref[...], preferred_element_type=jnp.float32).astype(jnp.bfloat16)

        @pl.when(is_end)
        def _():
            end_to_inner(c).start()

    def tick(tau):
        def live(c):
            return (c >= 0) & (c < n_chunks)

        def root(c):
            return 1 + lax.rem(c + 2 * n_chunks, 2)

        own = tau - jnp.where(is_relay, HOP_LAG, 0)
        arrives = is_relay & (lax.rem(own + 2 * n_chunks, 2) == 0)

        @pl.when(arrives & live(own))
        def _():
            to_partner(lax.div(own, 2)).wait_recv()

            @pl.when(is_end)
            def _():
                end_to_inner(own).start()

        first = own - HOP_LAG

        @pl.when(is_inner & live(first))
        def _():
            end_to_inner(first).wait_recv()

            @pl.when(t != root(first))
            def _():
                part[first] = (part[first].astype(jnp.float32) + ebuf[first].astype(jnp.float32)).astype(jnp.bfloat16)
                inner_to_peer(first).start()

        second = first - HOP_LAG

        @pl.when(is_inner & live(second) & (t == root(second)))
        def _():
            inner_to_peer(second).wait_recv()
            total = part[second].astype(jnp.float32) + ebuf[second].astype(jnp.float32) + ibuf[second].astype(jnp.float32)
            part[second] = total.astype(jnp.bfloat16)
            inner_to_peer(second).start()
            final_to_end(second, part).start()
            deliver(second, part)

        third = second - HOP_LAG

        @pl.when(is_inner & live(third) & (t != root(third)))
        def _():
            inner_to_peer(third).wait_recv()
            final_to_end(third, ibuf).start()
            deliver(third, ibuf)

        fourth = third - HOP_LAG

        @pl.when(is_end & live(fourth))
        def _():
            final_to_end(fourth, ibuf).wait_recv()
            deliver(fourth, ibuf)

    n_ticks = n_chunks + 5 * HOP_LAG

    def ticks_done(at):
        tile = at - n_heads_steps
        return jnp.where(tile < 0, 0, jnp.where(tile < n_tiles, 2 * (tile + 1), n_ticks))

    @pl.loop(ticks_done(step - 1), ticks_done(step))
    def _(tau):
        tick(tau)

    @pl.when(drain)
    def _():
        @pl.loop(0, n_chunks)
        def _(c):
            @pl.when(is_end)
            def _():
                end_to_inner(c).wait_send()

            @pl.when(is_inner)
            def _():
                inner_to_peer(c).wait_send()
                final_to_end(c, part).wait_send()

            @pl.when(is_prompt)
            def _():
                final_local(c, part).wait()
                final_back(c, part).wait_recv()

            @pl.when(is_relay)
            def _():
                final_back(c, part).wait_send()

        @pl.when(is_prompt)
        def _():
            cache_copy().wait_send()
            latent_over().wait_send()

            @pl.loop(0, n_tiles)
            def _(tile):
                to_partner(tile).wait_send()

            @pl.loop(0, n_pieces)
            def _(p):
                tokens_over(p).wait_send()

        @pl.when(is_relay)
        def _():
            cache_copy().wait_recv()
            latent_next(side).wait_send()

            @pl.loop(0, n_pieces)
            def _(p):
                tokens_next(p, side).wait_send()


def prefill(tokens, latent, padded, w_query, w_uk, w_uv, w_out, seq_len):
    rows, width = tokens.shape
    depth = w_out.shape[0]
    kv_rank = w_uk.shape[0]
    n_heads_steps = depth // (HEADS_STEP * V_DIM)
    n_tiles = width // TILE
    prompt_rows = rows - seq_len
    n_pieces = seq_len // 2 // PIECE

    def head_block(i):
        return jnp.minimum(i, n_heads_steps - 1)

    def tile_block(i):
        return jnp.clip(i - n_heads_steps, 0, n_tiles - 1)

    any_spec = pl.BlockSpec(memory_space=pl.ANY)
    tabs = lane_tables(seq_len)
    tab_spec = pl.BlockSpec((seq_len, 128), lambda i: (0, 0))
    chunk = pltpu.VMEM((2 * n_tiles, seq_len, TILE), jnp.bfloat16)
    sems = [n_pieces + 1] * 4 + [n_tiles] * 2 + [2 * n_tiles] * 8 + [2, 2]
    return pl.pallas_call(
        functools.partial(prefill_kernel, n_heads_steps, n_tiles),
        grid=(n_heads_steps + n_tiles + 1,),
        out_shape=(jax.ShapeDtypeStruct((rows, width), jnp.bfloat16), jax.ShapeDtypeStruct((seq_len, latent.shape[1]), jnp.bfloat16)),
        in_specs=[
            any_spec,
            pl.BlockSpec((width, HEADS_STEP * (NOPE_DIM + ROPE_DIM)), lambda i: (0, head_block(i))),
            pl.BlockSpec((kv_rank, HEADS_STEP * NOPE_DIM), lambda i: (0, head_block(i))),
            pl.BlockSpec((kv_rank, HEADS_STEP * V_DIM), lambda i: (0, head_block(i))),
            any_spec,
            tab_spec, tab_spec, tab_spec, tab_spec,
            pl.BlockSpec((depth, TILE), lambda i: (0, tile_block(i))),
            any_spec,
        ],
        out_specs=(any_spec, any_spec),
        scratch_shapes=[
            pltpu.VMEM((prompt_rows, width), jnp.bfloat16),
            pltpu.VMEM((prompt_rows, padded.shape[1]), jnp.bfloat16),
            pltpu.VMEM((2, prompt_rows, HEADS_STEP * (NOPE_DIM + ROPE_DIM)), jnp.bfloat16),
            pltpu.VMEM((2, prompt_rows, HEADS_STEP * NOPE_DIM), jnp.bfloat16),
            pltpu.VMEM((2, prompt_rows, HEADS_STEP * V_DIM), jnp.bfloat16),
            pltpu.VMEM((prompt_rows, depth), jnp.bfloat16),
            chunk,
            pltpu.VMEM((n_tiles, seq_len, TILE), jnp.bfloat16),
            chunk,
            chunk,
        ] + [pltpu.SemaphoreType.DMA((n,)) for n in sems],
        compiler_params=pltpu.CompilerParams(collective_id=0, has_side_effects=True, vmem_limit_bytes=67043328),
    )(tokens, w_query, w_uk, w_uv, padded, *tabs, w_out, latent)


def solution(mesh):
    half_stage = mesh.shape["stage"] // 2
    slot_spec = P(("dp", "stage"), None, None, None)
    cache_spec = P(("dp", "stage"), "t", None, None)

    def device_step(hidden, w_query, w_dkv, latent_gain, w_uk, w_uv, w_out):
        batch, seq_len, width = hidden.shape[1:]
        cos_tab, sin_tab = rope_tables(seq_len)
        latent = latent_rows(hidden[0], w_dkv, latent_gain, cos_tab, sin_tab).reshape(batch * seq_len, -1)
        padded = jnp.pad(latent, ((0, 0), (0, ROPE_DIM)))
        summed, handed = prefill(hidden.reshape(batch * seq_len, width), latent, padded, w_query, w_uk, w_uv, w_out, seq_len)
        is_prompt = lax.axis_index("stage") < half_stage
        out_rows = jnp.where(is_prompt, summed, jnp.zeros_like(summed)).reshape(1, batch, seq_len, width)
        cache = jnp.where(is_prompt, jnp.zeros_like(handed), handed)
        return out_rows, cache[None, None]

    return jax.shard_map(device_step, mesh=mesh, in_specs=(slot_spec, P(None, "t"), P(None, None), P(None), P(None, "t"), P(None, "t"), P("t", None)), out_specs=(slot_spec, cache_spec), check_vma=False)
```

```python
import functools

import jax
import jax.numpy as jnp
import numpy as np
from jax import lax
from jax.experimental import pallas as pl
from jax.experimental.pallas import tpu as pltpu
from jax.sharding import PartitionSpec as P

NOPE_DIM = 128
ROPE_DIM = 64
V_DIM = 128
NORM_EPS = 1e-6
ROPE_BASE = 10000.0
MESH = pl.DeviceIdType.MESH
TILE = 512
HOP_LAG = 2
HEADS_STEP = 4
PIECE = 16
SHIFTED = 2


def lane_tables(seq_len):
    half_dim = ROPE_DIM // 2
    inv_freq = np.float32(ROPE_BASE) ** (-np.arange(half_dim, dtype=np.float32) / np.float32(half_dim))
    angles = np.arange(seq_len, dtype=np.float32)[:, None] * inv_freq[None, :].astype(np.float32)
    cos_tab, sin_tab = np.cos(angles).astype(np.float32), np.sin(angles).astype(np.float32)
    one, zero = np.ones((seq_len, ROPE_DIM), np.float32), np.zeros((seq_len, ROPE_DIM), np.float32)
    cos_low = np.concatenate([cos_tab, cos_tab, one], axis=1)
    sin_low = np.concatenate([-sin_tab, sin_tab, zero], axis=1)
    cos_high = np.concatenate([one, cos_tab, cos_tab], axis=1)
    sin_high = np.concatenate([zero, -sin_tab, sin_tab], axis=1)
    return cos_low, sin_low, cos_high, sin_high


def rope_lanes(vecs, cos_tab, sin_tab, pick_up):
    as_f32 = vecs.astype(jnp.float32)
    turned = jnp.where(pick_up, pltpu.roll(as_f32, 96, 1), pltpu.roll(as_f32, 32, 1))
    return (as_f32 * cos_tab + turned * sin_tab).astype(jnp.bfloat16)


def project_heads(rows, slot, x_ref, w_buf, wuk_ref, wuv_ref, lat_ref, q_buf, k_buf, v_buf):
    kv_rank = wuk_ref.shape[0]
    q_buf[slot, :rows] = jnp.dot(x_ref[:rows], w_buf[slot], preferred_element_type=jnp.float32).astype(jnp.bfloat16)
    c_kv = lat_ref[:rows, :kv_rank]
    k_buf[slot, :rows] = jnp.dot(c_kv, wuk_ref[...], preferred_element_type=jnp.float32).astype(jnp.bfloat16)
    v_buf[slot, :rows] = jnp.dot(c_kv, wuv_ref[...], preferred_element_type=jnp.float32).astype(jnp.bfloat16)


def latent_heads(rows, x_ref, dkv_ref, gain_ref, cos_low, sin_low, lat_ref, lat_out, seq):
    kv_rank = gain_ref.shape[1]
    compressed = lax.dot_general(x_ref[:rows], dkv_ref[...], (((1,), (1,)), ((), ())), preferred_element_type=jnp.float32).astype(jnp.bfloat16)
    c_raw = compressed[:, :kv_rank].astype(jnp.float32)
    inv_rms = lax.rsqrt(jnp.mean(c_raw * c_raw, axis=1, keepdims=True) + NORM_EPS)
    c_kv = (c_raw * inv_rms * gain_ref[...].astype(jnp.float32)).astype(jnp.bfloat16)
    lat_ref[:rows, :kv_rank] = c_kv
    lat_out[:rows, :kv_rank] = c_kv
    pick_up = (lax.broadcasted_iota(jnp.int32, (seq, 128), 1) & 32) == 0
    wide = jnp.concatenate([compressed[:, kv_rank:], jnp.zeros((rows, ROPE_DIM), jnp.bfloat16)], axis=1)
    for req in range(rows // seq):
        here = slice(req * seq, (req + 1) * seq)
        turned = rope_lanes(wide[here], cos_low[...], sin_low[...], pick_up)
        lat_ref[here, kv_rank:] = turned
        lat_out[here, kv_rank:] = turned[:, :ROPE_DIM]


def attend_request(q_ref, k_ref, v_ref, lat_ref, tabs, here, seq):
    kv_rank = lat_ref.shape[1] - 128
    cos_low, sin_low, cos_high, sin_high = (tab[...] for tab in tabs)
    lane = lax.broadcasted_iota(jnp.int32, (seq, 128), 1)
    low = lane < 64
    pick_up = (lane & 32) == 0
    key_rope = lat_ref[here, kv_rank:]
    key_rope_high = pltpu.roll(key_rope.astype(jnp.float32), 64, 1)
    causal = lax.broadcasted_iota(jnp.int32, (seq, seq), 1) <= lax.broadcasted_iota(jnp.int32, (seq, seq), 0)
    scale = (NOPE_DIM + ROPE_DIM) ** -0.5
    all_scores = []
    for pair in range(HEADS_STEP // 2):
        base = 384 * pair
        q_a = q_ref[here, base:base + 128]
        q_b = rope_lanes(q_ref[here, base + 128:base + 256], cos_low, sin_low, pick_up)
        q_c = rope_lanes(q_ref[here, base + 256:base + 384], cos_high, sin_high, pick_up)
        k_even = k_ref[here, 256 * pair:256 * pair + 128]
        k_odd = pltpu.roll(k_ref[here, 256 * pair + 128:256 * pair + 256].astype(jnp.float32), 64, 1)
        k_odd_a = jnp.where(low, 0.0, k_odd).astype(jnp.bfloat16)
        k_odd_b = jnp.where(low, k_odd, key_rope_high).astype(jnp.bfloat16)
        sides = ((jnp.concatenate([q_a, q_b], axis=1), jnp.concatenate([k_even, key_rope], axis=1)),
                 (jnp.concatenate([q_b, q_c], axis=1), jnp.concatenate([k_odd_a, k_odd_b], axis=1)))
        for q_side, k_side in sides:
            all_scores.append(lax.dot_general(q_side, k_side, (((1,), (1,)), ((), ())), preferred_element_type=jnp.float32))
    mixes = []
    for head, scores in enumerate(all_scores):
        scores = jnp.where(causal, scores * scale, -jnp.inf)
        weights = jnp.exp(scores - jnp.max(scores, axis=1, keepdims=True))
        total = jnp.sum(weights, axis=1, keepdims=True)
        mixed = jnp.dot(weights.astype(jnp.bfloat16), v_ref[here, 128 * head:128 * head + 128], preferred_element_type=jnp.float32)
        mixes.append((mixed / total).astype(jnp.bfloat16))
    return jnp.concatenate(mixes, axis=1)


def prefill_kernel(n_heads_steps, n_tiles, x_src, wq_src, wuk_ref, wuv_ref, gain_ref, tab_a, tab_b, tab_c, tab_d, wout_src, dkv_src,
                   out_ref, cache_ref, x_ref, w_buf, dkv_ref, lat_ref, lat_out, q_buf, k_buf, v_buf, heads_out, part, partb, ebuf, ibuf,
                   send_x, recv_x, send_n, recv_n, send_b, recv_p, send_e, recv_e, send_i, recv_i, send_f, send_o, recv_o, local_sem, lat_sem, load_sem, w_sem):
    step = pl.program_id(0)
    n_line1 = 2 * n_tiles
    n_chunks = n_line1 + SHIFTED
    kept = n_tiles - SHIFTED
    t = lax.axis_index("t")
    stage = lax.axis_index("stage")
    is_prompt = stage < 2
    is_relay = stage >= 2
    partner = lax.rem(stage + 2, 4)
    is_end = (t == 0) | (t == 3)
    is_inner = (t == 1) | (t == 2)
    peer = 3 - t
    inner_nb = jnp.where(t == 0, 1, 2)
    end_nb = jnp.where(t == 1, 0, 3)
    pair_nb = jnp.where(is_end, inner_nb, end_nb)
    seq = cache_ref.shape[0]
    prompt_rows = x_ref.shape[0]
    half = seq // 2
    side = lax.rem(t, 2)
    n_pieces = half // PIECE
    drain = step == n_heads_steps + n_tiles
    in_heads = step < n_heads_steps
    in_tiles = (step >= n_heads_steps) & (step < n_heads_steps + n_tiles)

    def tokens_over(p):
        src = pl.multiple_of(prompt_rows + side * half + p * PIECE, PIECE)
        dst = pl.multiple_of(side * half + p * PIECE, PIECE)
        return pltpu.make_async_remote_copy(src_ref=x_src.at[pl.ds(src, PIECE)], dst_ref=x_ref.at[pl.ds(dst, PIECE)], send_sem=send_x.at[p],
                                            recv_sem=recv_x.at[p], device_id={"stage": partner}, device_id_type=MESH)

    def tokens_next(p, which):
        rows = pl.ds(pl.multiple_of(which * half + p * PIECE, PIECE), PIECE)
        return pltpu.make_async_remote_copy(src_ref=x_ref.at[rows], dst_ref=x_ref.at[rows], send_sem=send_n.at[p],
                                            recv_sem=recv_n.at[p], device_id={"t": pair_nb}, device_id_type=MESH)

    def to_partner(tile):
        return pltpu.make_async_remote_copy(src_ref=partb.at[tile], dst_ref=part.at[2 * tile], send_sem=send_b.at[tile], recv_sem=recv_p.at[tile],
                                            device_id={"stage": partner}, device_id_type=MESH)

    def end_to_inner(c):
        return pltpu.make_async_remote_copy(src_ref=part.at[c], dst_ref=ebuf.at[c], send_sem=send_e.at[c], recv_sem=recv_e.at[c],
                                            device_id={"t": inner_nb}, device_id_type=MESH)

    def inner_to_peer(c):
        return pltpu.make_async_remote_copy(src_ref=part.at[c], dst_ref=ibuf.at[c], send_sem=send_i.at[c], recv_sem=recv_i.at[c],
                                            device_id={"t": peer}, device_id_type=MESH)

    def final_to_end(c):
        return pltpu.make_async_remote_copy(src_ref=ebuf.at[c], dst_ref=ibuf.at[c], send_sem=send_f.at[c], recv_sem=recv_i.at[c],
                                            device_id={"t": end_nb}, device_id_type=MESH)

    def place(c, line):
        extra = c >= n_line1
        row = jnp.where(extra, 2, 2 * line + lax.rem(c, 2)) * seq
        col = jnp.where(extra, kept + c - n_line1, lax.div(c, 2)) * TILE
        return out_ref.at[pl.ds(pl.multiple_of(row, seq), seq), pl.ds(pl.multiple_of(col, TILE), TILE)]

    def final_back(c, src):
        return pltpu.make_async_remote_copy(src_ref=src.at[c], dst_ref=place(c, 1), send_sem=send_o.at[c],
                                            recv_sem=recv_o.at[c], device_id={"stage": partner}, device_id_type=MESH)

    def final_local(c, src):
        return pltpu.make_async_copy(src.at[c], place(c, 0), local_sem.at[c])

    def cache_copy():
        return pltpu.make_async_remote_copy(src_ref=lat_out.at[pl.ds(pl.multiple_of(t * seq, seq), seq)], dst_ref=cache_ref, send_sem=lat_sem.at[0],
                                            recv_sem=lat_sem.at[1], device_id={"stage": partner}, device_id_type=MESH)

    def cache_own():
        return pltpu.make_async_copy(lat_out.at[pl.ds(0, seq)], cache_ref, lat_sem.at[0])

    def on_line(c):
        moved = (c >= 2 * kept) & (lax.rem(c + 2 * n_chunks, 2) == 0)
        return (c >= 0) & ((is_prompt & (c < n_chunks)) | (is_relay & (c < n_line1) & jnp.logical_not(moved)))

    def on_relay_line(c):
        return (c < n_line1) & jnp.logical_not((c >= 2 * kept) & (lax.rem(c, 2) == 0))

    def load_q(i):
        width = w_buf.shape[2]
        return pltpu.make_async_copy(wq_src.at[:, pl.ds(pl.multiple_of(i * width, width), width)], w_buf.at[lax.rem(i, 2)], w_sem.at[lax.rem(i, 2)])

    def load_out(k):
        slot = lax.rem(k + n_heads_steps, 2)
        return pltpu.make_async_copy(wout_src.at[:, pl.ds(pl.multiple_of(k * TILE, TILE), TILE)],
                                     w_buf.at[slot, pl.ds(0, heads_out.shape[1]), pl.ds(0, TILE)], w_sem.at[slot])

    def load_x():
        return pltpu.make_async_copy(x_src.at[pl.ds(0, prompt_rows)], x_ref, load_sem.at[0])

    def load_dkv():
        return pltpu.make_async_copy(dkv_src, dkv_ref, load_sem.at[1])

    def deliver(c, src):
        @pl.when(is_prompt)
        def _():
            final_local(c, src).start()

        @pl.when(is_relay)
        def _():
            final_back(c, src).start()

    @pl.when(step == 0)
    def _():
        @pl.when(is_prompt)
        def _():
            load_x().start()

        load_dkv().start()
        load_q(0).start()
        barrier = pltpu.get_barrier_semaphore()
        pl.semaphore_signal(barrier, inc=1, device_id={"stage": partner}, device_id_type=MESH)

        @pl.when(is_end)
        def _():
            pl.semaphore_signal(barrier, inc=1, device_id={"t": inner_nb}, device_id_type=MESH)
            pl.semaphore_wait(barrier, 2)

        @pl.when(is_inner)
        def _():
            pl.semaphore_signal(barrier, inc=1, device_id={"t": end_nb}, device_id_type=MESH)
            pl.semaphore_signal(barrier, inc=1, device_id={"t": peer}, device_id_type=MESH)
            pl.semaphore_wait(barrier, 3)

        @pl.when(is_prompt)
        def _():
            @pl.loop(0, n_pieces)
            def _(p):
                tokens_over(p).start()

            load_x().wait()
            load_dkv().wait()
            latent_heads(prompt_rows, x_ref, dkv_ref, gain_ref, tab_a, tab_b, lat_ref, lat_out, seq)

        @pl.when(is_relay)
        def _():
            @pl.loop(0, n_pieces)
            def _(p):
                tokens_over(p).wait_recv()
                tokens_next(p, side).start()

            load_dkv().wait()

            @pl.loop(0, n_pieces)
            def _(p):
                tokens_next(p, 1 - side).wait_recv()

            latent_heads(seq, x_ref, dkv_ref, gain_ref, tab_a, tab_b, lat_ref, lat_out, seq)

    @pl.when(step + 1 < n_heads_steps)
    def _():
        load_q(step + 1).start()

    @pl.when((step + 1 >= n_heads_steps) & (step + 1 < n_heads_steps + n_tiles))
    def _():
        load_out(step + 1 - n_heads_steps).start()

    @pl.when(in_heads)
    def _():
        load_q(step).wait()

    @pl.when(in_tiles)
    def _():
        load_out(step - n_heads_steps).wait()

    def attend(rows):
        width = HEADS_STEP * V_DIM
        slot = lax.rem(step + 1, 2)
        done = lax.rem(step + n_heads_steps - 1, n_heads_steps)
        for req in range(rows // seq):
            here = slice(req * seq, (req + 1) * seq)
            heads_out[here, pl.ds(pl.multiple_of(done * width, width), width)] = attend_request(
                q_buf.at[slot], k_buf.at[slot], v_buf.at[slot], lat_ref, (tab_a, tab_b, tab_c, tab_d), here, seq)

    for mine, rows in ((is_prompt, prompt_rows), (is_relay, seq)):
        @pl.when(mine & in_heads)
        def _():
            attend(rows)
            project_heads(rows, lax.rem(step, 2), x_ref, w_buf, wuk_ref, wuv_ref, lat_ref, q_buf, k_buf, v_buf)

        @pl.when(mine & (step == n_heads_steps))
        def _():
            attend(rows)

    @pl.when(is_prompt & (step == n_heads_steps) & (t < 3))
    def _():
        cache_copy().start()

    @pl.when(is_relay & (step == n_heads_steps) & (t == 3))
    def _():
        cache_own().start()

    def out_block():
        return w_buf[lax.rem(step, 2), :heads_out.shape[1], :TILE]

    @pl.when(is_prompt & in_tiles)
    def _():
        tile = step - n_heads_steps
        full = jnp.dot(heads_out[...], out_block(), preferred_element_type=jnp.float32).astype(jnp.bfloat16)
        part[2 * tile] = full[:seq]
        part[2 * tile + 1] = full[seq:2 * seq]

        @pl.when(tile < kept)
        def _():
            partb[tile] = full[2 * seq:]
            to_partner(tile).start()

        @pl.when(tile >= kept)
        def _():
            part[n_line1 + tile - kept] = full[2 * seq:]

        @pl.when(is_end)
        def _():
            end_to_inner(2 * tile).start()
            end_to_inner(2 * tile + 1).start()

            @pl.when(tile >= kept)
            def _():
                end_to_inner(n_line1 + tile - kept).start()

    @pl.when(is_relay & in_tiles)
    def _():
        c = 2 * (step - n_heads_steps) + 1
        part[c] = jnp.dot(heads_out[:seq], out_block(), preferred_element_type=jnp.float32).astype(jnp.bfloat16)

        @pl.when(is_end)
        def _():
            end_to_inner(c).start()

    def tick(tau):
        own = tau - jnp.where(is_relay, HOP_LAG, 0)
        arrives = is_relay & (lax.rem(own + 2 * n_chunks, 2) == 0)

        @pl.when(arrives & on_line(own))
        def _():
            to_partner(lax.div(own, 2)).wait_recv()

            @pl.when(is_end)
            def _():
                end_to_inner(own).start()

        first = own - HOP_LAG

        @pl.when(is_inner & on_line(first))
        def _():
            end_to_inner(first).wait_recv()

            part[first] = (part[first].astype(jnp.float32) + ebuf[first].astype(jnp.float32)).astype(jnp.bfloat16)
            inner_to_peer(first).start()

        second = first - HOP_LAG

        @pl.when(is_inner & on_line(second))
        def _():
            inner_to_peer(second).wait_recv()
            ebuf[second] = (part[second].astype(jnp.float32) + ibuf[second].astype(jnp.float32)).astype(jnp.bfloat16)
            final_to_end(second).start()
            deliver(second, ebuf)

        third = second - HOP_LAG

        @pl.when(is_end & on_line(third))
        def _():
            final_to_end(third).wait_recv()
            deliver(third, ibuf)

    n_ticks = max(n_chunks + 3 * HOP_LAG, n_line1 + 4 * HOP_LAG)

    def ticks_done(at):
        tile = at - n_heads_steps
        return jnp.where(tile < 0, 0, jnp.where(tile < n_tiles, 2 * (tile + 1), n_ticks))

    @pl.loop(ticks_done(step - 1), ticks_done(step))
    def _(tau):
        tick(tau)

    @pl.when(drain)
    def _():
        @pl.loop(0, n_chunks)
        def _(c):
            @pl.when(is_end & on_line(c))
            def _():
                end_to_inner(c).wait_send()

            @pl.when(is_inner & on_line(c))
            def _():
                inner_to_peer(c).wait_send()
                final_to_end(c).wait_send()

            @pl.when(is_prompt)
            def _():
                final_local(c, part).wait()

            @pl.when(is_prompt & on_relay_line(c))
            def _():
                final_back(c, part).wait_recv()

            @pl.when(is_relay & on_line(c))
            def _():
                final_back(c, part).wait_send()

        @pl.when(is_prompt)
        def _():
            @pl.when(t < 3)
            def _():
                cache_copy().wait_send()

            @pl.loop(0, kept)
            def _(tile):
                to_partner(tile).wait_send()

            @pl.loop(0, n_pieces)
            def _(p):
                tokens_over(p).wait_send()

        @pl.when(is_relay)
        def _():
            @pl.when(t < 3)
            def _():
                cache_copy().wait_recv()

            @pl.when(t == 3)
            def _():
                cache_own().wait()

            @pl.loop(0, n_pieces)
            def _(p):
                tokens_next(p, side).wait_send()


def prefill(tokens, w_query, w_dkv, gain, w_uk, w_uv, w_out, seq_len):
    rows, width = tokens.shape
    depth = w_out.shape[0]
    kv_rank = w_uk.shape[0]
    n_heads_steps = depth // (HEADS_STEP * V_DIM)
    n_tiles = width // TILE
    prompt_rows = rows - seq_len
    latent_width = w_dkv.shape[0]
    n_pieces = seq_len // 2 // PIECE

    def head_block(i):
        return jnp.minimum(i, n_heads_steps - 1)

    any_spec = pl.BlockSpec(memory_space=pl.ANY)
    tabs = lane_tables(seq_len)
    tab_spec = pl.BlockSpec((seq_len, 128), lambda i: (0, 0))
    chunk = pltpu.VMEM((2 * n_tiles + SHIFTED, seq_len, TILE), jnp.bfloat16)
    sems = [n_pieces] * 4 + [n_tiles] * 2 + [2 * n_tiles + SHIFTED] * 8 + [2, 2, 2]
    return pl.pallas_call(
        functools.partial(prefill_kernel, n_heads_steps, n_tiles),
        grid=(n_heads_steps + n_tiles + 1,),
        out_shape=(jax.ShapeDtypeStruct((rows, width), jnp.bfloat16), jax.ShapeDtypeStruct((seq_len, latent_width), jnp.bfloat16)),
        in_specs=[
            any_spec,
            any_spec,
            pl.BlockSpec((kv_rank, HEADS_STEP * NOPE_DIM), lambda i: (0, head_block(i))),
            pl.BlockSpec((kv_rank, HEADS_STEP * V_DIM), lambda i: (0, head_block(i))),
            pl.BlockSpec((1, kv_rank), lambda i: (0, 0)),
            tab_spec, tab_spec, tab_spec, tab_spec,
            any_spec,
            any_spec,
        ],
        out_specs=(any_spec, any_spec),
        scratch_shapes=[
            pltpu.VMEM((prompt_rows, width), jnp.bfloat16),
            pltpu.VMEM((2, width, HEADS_STEP * (NOPE_DIM + ROPE_DIM)), jnp.bfloat16),
            pltpu.VMEM((latent_width, width), jnp.bfloat16),
            pltpu.VMEM((prompt_rows, kv_rank + 128), jnp.bfloat16),
            pltpu.VMEM((prompt_rows, latent_width), jnp.bfloat16),
            pltpu.VMEM((2, prompt_rows, HEADS_STEP * (NOPE_DIM + ROPE_DIM)), jnp.bfloat16),
            pltpu.VMEM((2, prompt_rows, HEADS_STEP * NOPE_DIM), jnp.bfloat16),
            pltpu.VMEM((2, prompt_rows, HEADS_STEP * V_DIM), jnp.bfloat16),
            pltpu.VMEM((prompt_rows, depth), jnp.bfloat16),
            chunk,
            pltpu.VMEM((n_tiles, seq_len, TILE), jnp.bfloat16),
            chunk,
            chunk,
        ] + [pltpu.SemaphoreType.DMA((n,)) for n in sems],
        compiler_params=pltpu.CompilerParams(collective_id=0, has_side_effects=True, vmem_limit_bytes=67043328),
    )(tokens, w_query, w_uk, w_uv, gain, *tabs, w_out, w_dkv)


def solution(mesh):
    half_stage = mesh.shape["stage"] // 2
    slot_spec = P(("dp", "stage"), None, None, None)
    cache_spec = P(("dp", "stage"), "t", None, None)

    def device_step(hidden, w_query, w_dkv, latent_gain, w_uk, w_uv, w_out):
        batch, seq_len, width = hidden.shape[1:]
        summed, handed = prefill(hidden.reshape(batch * seq_len, width), w_query, w_dkv.T, latent_gain[None], w_uk, w_uv, w_out, seq_len)
        is_prompt = lax.axis_index("stage") < half_stage
        out_rows = jnp.where(is_prompt, summed, jnp.zeros_like(summed)).reshape(1, batch, seq_len, width)
        cache = jnp.where(is_prompt, jnp.zeros_like(handed), handed)
        return out_rows, cache[None, None]

    return jax.shard_map(device_step, mesh=mesh, in_specs=(slot_spec, P(None, "t"), P(None, None), P(None), P(None, "t"), P(None, "t"), P("t", None)), out_specs=(slot_spec, cache_spec), check_vma=False)
```

```python
import functools

import jax
import jax.numpy as jnp
import numpy as np
from jax import lax
from jax.experimental import pallas as pl
from jax.experimental.pallas import tpu as pltpu
from jax.sharding import PartitionSpec as P

NOPE_DIM = 128
ROPE_DIM = 64
V_DIM = 128
NORM_EPS = 1e-6
ROPE_BASE = 10000.0
MESH = pl.DeviceIdType.MESH
TILE = 512
HOP_LAG = 2
HEADS_STEP = 4
PIECE = 16
SHIFTED = 1


def lane_tables(seq_len):
    half_dim = ROPE_DIM // 2
    inv_freq = np.float32(ROPE_BASE) ** (-np.arange(half_dim, dtype=np.float32) / np.float32(half_dim))
    angles = np.arange(seq_len, dtype=np.float32)[:, None] * inv_freq[None, :].astype(np.float32)
    cos_tab, sin_tab = np.cos(angles).astype(np.float32), np.sin(angles).astype(np.float32)
    one, zero = np.ones((seq_len, ROPE_DIM), np.float32), np.zeros((seq_len, ROPE_DIM), np.float32)
    cos_low = np.concatenate([cos_tab, cos_tab, one], axis=1)
    sin_low = np.concatenate([-sin_tab, sin_tab, zero], axis=1)
    cos_high = np.concatenate([one, cos_tab, cos_tab], axis=1)
    sin_high = np.concatenate([zero, -sin_tab, sin_tab], axis=1)
    return cos_low, sin_low, cos_high, sin_high


def rope_lanes(vecs, cos_tab, sin_tab, pick_up):
    as_f32 = vecs.astype(jnp.float32)
    turned = jnp.where(pick_up, pltpu.roll(as_f32, 96, 1), pltpu.roll(as_f32, 32, 1))
    return (as_f32 * cos_tab + turned * sin_tab).astype(jnp.bfloat16)


def project_heads(rows, slot, x_ref, w_buf, wuk_ref, wuv_ref, lat_ref, q_buf, k_buf, v_buf):
    kv_rank = wuk_ref.shape[0]
    q_buf[slot, :rows] = jnp.dot(x_ref[:rows], w_buf[slot], preferred_element_type=jnp.float32).astype(jnp.bfloat16)
    c_kv = lat_ref[:rows, :kv_rank]
    k_buf[slot, :rows] = jnp.dot(c_kv, wuk_ref[...], preferred_element_type=jnp.float32).astype(jnp.bfloat16)
    v_buf[slot, :rows] = jnp.dot(c_kv, wuv_ref[...], preferred_element_type=jnp.float32).astype(jnp.bfloat16)


def latent_heads(rows, x_ref, dkv_ref, gain_ref, cos_low, sin_low, lat_ref, lat_out, seq):
    kv_rank = gain_ref.shape[0]
    compressed = lax.dot_general(x_ref[:rows], dkv_ref[...], (((1,), (1,)), ((), ())), preferred_element_type=jnp.float32).astype(jnp.bfloat16)
    c_raw = compressed[:, :kv_rank].astype(jnp.float32)
    inv_rms = lax.rsqrt(jnp.mean(c_raw * c_raw, axis=1, keepdims=True) + NORM_EPS)
    c_kv = (c_raw * inv_rms * gain_ref[...].astype(jnp.float32)[None, :]).astype(jnp.bfloat16)
    lat_ref[:rows, :kv_rank] = c_kv
    lat_out[:rows, :kv_rank] = c_kv
    pick_up = (lax.broadcasted_iota(jnp.int32, (seq, 128), 1) & 32) == 0
    wide = jnp.concatenate([compressed[:, kv_rank:], jnp.zeros((rows, ROPE_DIM), jnp.bfloat16)], axis=1)
    for req in range(rows // seq):
        here = slice(req * seq, (req + 1) * seq)
        turned = rope_lanes(wide[here], cos_low[...], sin_low[...], pick_up)
        lat_ref[here, kv_rank:] = turned
        lat_out[here, kv_rank:] = turned[:, :ROPE_DIM]


def attend_request(q_ref, k_ref, v_ref, lat_ref, tabs, here, seq):
    kv_rank = lat_ref.shape[1] - 128
    cos_low, sin_low, cos_high, sin_high = (tab[...] for tab in tabs)
    lane = lax.broadcasted_iota(jnp.int32, (seq, 128), 1)
    low = lane < 64
    pick_up = (lane & 32) == 0
    key_rope = lat_ref[here, kv_rank:]
    key_rope_high = pltpu.roll(key_rope.astype(jnp.float32), 64, 1)
    causal = lax.broadcasted_iota(jnp.int32, (seq, seq), 1) <= lax.broadcasted_iota(jnp.int32, (seq, seq), 0)
    scale = (NOPE_DIM + ROPE_DIM) ** -0.5
    all_scores = []
    for pair in range(HEADS_STEP // 2):
        base = 384 * pair
        q_a = q_ref[here, base:base + 128]
        q_b = rope_lanes(q_ref[here, base + 128:base + 256], cos_low, sin_low, pick_up)
        q_c = rope_lanes(q_ref[here, base + 256:base + 384], cos_high, sin_high, pick_up)
        k_even = k_ref[here, 256 * pair:256 * pair + 128]
        k_odd = pltpu.roll(k_ref[here, 256 * pair + 128:256 * pair + 256].astype(jnp.float32), 64, 1)
        k_odd_a = jnp.where(low, 0.0, k_odd).astype(jnp.bfloat16)
        k_odd_b = jnp.where(low, k_odd, key_rope_high).astype(jnp.bfloat16)
        sides = ((jnp.concatenate([q_a, q_b], axis=1), jnp.concatenate([k_even, key_rope], axis=1)),
                 (jnp.concatenate([q_b, q_c], axis=1), jnp.concatenate([k_odd_a, k_odd_b], axis=1)))
        for q_side, k_side in sides:
            all_scores.append(lax.dot_general(q_side, k_side, (((1,), (1,)), ((), ())), preferred_element_type=jnp.float32))
    mixes = []
    for head, scores in enumerate(all_scores):
        scores = jnp.where(causal, scores * scale, -jnp.inf)
        weights = jnp.exp(scores - jnp.max(scores, axis=1, keepdims=True))
        total = jnp.sum(weights, axis=1, keepdims=True)
        mixed = jnp.dot(weights.astype(jnp.bfloat16), v_ref[here, 128 * head:128 * head + 128], preferred_element_type=jnp.float32)
        mixes.append((mixed / total).astype(jnp.bfloat16))
    return jnp.concatenate(mixes, axis=1)


def prefill_kernel(n_heads_steps, n_tiles, x_src, wq_src, wuk_ref, wuv_ref, gain_ref, tab_a, tab_b, tab_c, tab_d, wout_src, dkv_src,
                   out_ref, cache_ref, x_ref, w_buf, dkv_ref, lat_ref, lat_out, q_buf, k_buf, v_buf, heads_out, part, partb, ebuf, ibuf,
                   send_x, recv_x, send_n, recv_n, send_b, recv_p, send_e, recv_e, send_i, recv_i, send_f, send_o, recv_o, local_sem, lat_sem, load_sem, w_sem):
    step = pl.program_id(0)
    n_line1 = 2 * n_tiles
    n_chunks = n_line1 + SHIFTED
    kept = n_tiles - SHIFTED
    t = lax.axis_index("t")
    stage = lax.axis_index("stage")
    is_prompt = stage < 2
    is_relay = stage >= 2
    partner = lax.rem(stage + 2, 4)
    is_end = (t == 0) | (t == 3)
    is_inner = (t == 1) | (t == 2)
    peer = 3 - t
    inner_nb = jnp.where(t == 0, 1, 2)
    end_nb = jnp.where(t == 1, 0, 3)
    pair_nb = jnp.where(is_end, inner_nb, end_nb)
    seq = cache_ref.shape[0]
    prompt_rows = x_ref.shape[0]
    half = seq // 2
    side = lax.rem(t, 2)
    n_pieces = half // PIECE
    drain = step == n_heads_steps + n_tiles
    in_heads = step < n_heads_steps
    in_tiles = (step >= n_heads_steps) & (step < n_heads_steps + n_tiles)

    def tokens_over(p):
        src = pl.multiple_of(prompt_rows + side * half + p * PIECE, PIECE)
        dst = pl.multiple_of(side * half + p * PIECE, PIECE)
        return pltpu.make_async_remote_copy(src_ref=x_src.at[pl.ds(src, PIECE)], dst_ref=x_ref.at[pl.ds(dst, PIECE)], send_sem=send_x.at[p],
                                            recv_sem=recv_x.at[p], device_id={"stage": partner}, device_id_type=MESH)

    def tokens_next(p, which):
        rows = pl.ds(pl.multiple_of(which * half + p * PIECE, PIECE), PIECE)
        return pltpu.make_async_remote_copy(src_ref=x_ref.at[rows], dst_ref=x_ref.at[rows], send_sem=send_n.at[p],
                                            recv_sem=recv_n.at[p], device_id={"t": pair_nb}, device_id_type=MESH)

    def to_partner(tile):
        return pltpu.make_async_remote_copy(src_ref=partb.at[tile], dst_ref=part.at[2 * tile], send_sem=send_b.at[tile], recv_sem=recv_p.at[tile],
                                            device_id={"stage": partner}, device_id_type=MESH)

    def end_to_inner(c):
        return pltpu.make_async_remote_copy(src_ref=part.at[c], dst_ref=ebuf.at[c], send_sem=send_e.at[c], recv_sem=recv_e.at[c],
                                            device_id={"t": inner_nb}, device_id_type=MESH)

    def inner_to_peer(c):
        return pltpu.make_async_remote_copy(src_ref=part.at[c], dst_ref=ibuf.at[c], send_sem=send_i.at[c], recv_sem=recv_i.at[c],
                                            device_id={"t": peer}, device_id_type=MESH)

    def final_to_end(c):
        return pltpu.make_async_remote_copy(src_ref=ebuf.at[c], dst_ref=ibuf.at[c], send_sem=send_f.at[c], recv_sem=recv_i.at[c],
                                            device_id={"t": end_nb}, device_id_type=MESH)

    def place(c, line):
        extra = c >= n_line1
        row = jnp.where(extra, 2, 2 * line + lax.rem(c, 2)) * seq
        col = jnp.where(extra, kept + c - n_line1, lax.div(c, 2)) * TILE
        return out_ref.at[pl.ds(pl.multiple_of(row, seq), seq), pl.ds(pl.multiple_of(col, TILE), TILE)]

    def final_back(c, src):
        return pltpu.make_async_remote_copy(src_ref=src.at[c], dst_ref=place(c, 1), send_sem=send_o.at[c],
                                            recv_sem=recv_o.at[c], device_id={"stage": partner}, device_id_type=MESH)

    def final_local(c, src):
        return pltpu.make_async_copy(src.at[c], place(c, 0), local_sem.at[c])

    def cache_copy():
        return pltpu.make_async_remote_copy(src_ref=lat_out.at[pl.ds(pl.multiple_of(t * seq, seq), seq)], dst_ref=cache_ref, send_sem=lat_sem.at[0],
                                            recv_sem=lat_sem.at[1], device_id={"stage": partner}, device_id_type=MESH)

    def cache_own():
        return pltpu.make_async_copy(lat_out.at[pl.ds(0, seq)], cache_ref, lat_sem.at[0])

    def on_line(c):
        moved = (c >= 2 * kept) & (lax.rem(c + 2 * n_chunks, 2) == 0)
        return (c >= 0) & ((is_prompt & (c < n_chunks)) | (is_relay & (c < n_line1) & jnp.logical_not(moved)))

    def on_relay_line(c):
        return (c < n_line1) & jnp.logical_not((c >= 2 * kept) & (lax.rem(c, 2) == 0))

    def load_q(i):
        width = w_buf.shape[2]
        return pltpu.make_async_copy(wq_src.at[:, pl.ds(pl.multiple_of(i * width, width), width)], w_buf.at[lax.rem(i, 2)], w_sem.at[lax.rem(i, 2)])

    def load_out(k):
        slot = lax.rem(k + n_heads_steps, 2)
        return pltpu.make_async_copy(wout_src.at[:, pl.ds(pl.multiple_of(k * TILE, TILE), TILE)],
                                     w_buf.at[slot, pl.ds(0, heads_out.shape[1]), pl.ds(0, TILE)], w_sem.at[slot])

    def load_x():
        return pltpu.make_async_copy(x_src.at[pl.ds(0, prompt_rows)], x_ref, load_sem.at[0])

    def load_dkv():
        return pltpu.make_async_copy(dkv_src, dkv_ref, load_sem.at[1])

    def deliver(c, src):
        @pl.when(is_prompt)
        def _():
            final_local(c, src).start()

        @pl.when(is_relay)
        def _():
            final_back(c, src).start()

    @pl.when(step == 0)
    def _():
        @pl.when(is_prompt)
        def _():
            load_x().start()

        load_dkv().start()
        barrier = pltpu.get_barrier_semaphore()
        pl.semaphore_signal(barrier, inc=1, device_id={"stage": partner}, device_id_type=MESH)

        @pl.when(is_end)
        def _():
            pl.semaphore_signal(barrier, inc=1, device_id={"t": inner_nb}, device_id_type=MESH)
            pl.semaphore_wait(barrier, 2)

        @pl.when(is_inner)
        def _():
            pl.semaphore_signal(barrier, inc=1, device_id={"t": end_nb}, device_id_type=MESH)
            pl.semaphore_signal(barrier, inc=1, device_id={"t": peer}, device_id_type=MESH)
            pl.semaphore_wait(barrier, 3)

        @pl.when(is_prompt)
        def _():
            @pl.loop(0, n_pieces)
            def _(p):
                tokens_over(p).start()

            load_x().wait()
            load_dkv().wait()
            load_q(0).start()
            latent_heads(prompt_rows, x_ref, dkv_ref, gain_ref, tab_a, tab_b, lat_ref, lat_out, seq)

        @pl.when(is_relay)
        def _():
            @pl.loop(0, n_pieces)
            def _(p):
                tokens_over(p).wait_recv()
                tokens_next(p, side).start()

            load_dkv().wait()
            load_q(0).start()

            @pl.loop(0, n_pieces)
            def _(p):
                tokens_next(p, 1 - side).wait_recv()

            latent_heads(seq, x_ref, dkv_ref, gain_ref, tab_a, tab_b, lat_ref, lat_out, seq)

    @pl.when(step + 1 < n_heads_steps)
    def _():
        load_q(step + 1).start()

    @pl.when((step + 1 >= n_heads_steps) & (step + 1 < n_heads_steps + n_tiles))
    def _():
        load_out(step + 1 - n_heads_steps).start()

    @pl.when(in_heads)
    def _():
        load_q(step).wait()

    @pl.when(in_tiles)
    def _():
        load_out(step - n_heads_steps).wait()

    def attend(rows):
        width = HEADS_STEP * V_DIM
        slot = lax.rem(step + 1, 2)
        done = lax.rem(step + n_heads_steps - 1, n_heads_steps)
        for req in range(rows // seq):
            here = slice(req * seq, (req + 1) * seq)
            heads_out[here, pl.ds(pl.multiple_of(done * width, width), width)] = attend_request(
                q_buf.at[slot], k_buf.at[slot], v_buf.at[slot], lat_ref, (tab_a, tab_b, tab_c, tab_d), here, seq)

    for mine, rows in ((is_prompt, prompt_rows), (is_relay, seq)):
        @pl.when(mine & in_heads)
        def _():
            attend(rows)
            project_heads(rows, lax.rem(step, 2), x_ref, w_buf, wuk_ref, wuv_ref, lat_ref, q_buf, k_buf, v_buf)

        @pl.when(mine & (step == n_heads_steps))
        def _():
            attend(rows)

    @pl.when(is_prompt & (step == n_heads_steps) & (t < 3))
    def _():
        cache_copy().start()

    @pl.when(is_relay & (step == n_heads_steps) & (t == 3))
    def _():
        cache_own().start()

    def out_block():
        return w_buf[lax.rem(step, 2), :heads_out.shape[1], :TILE]

    @pl.when(is_prompt & in_tiles)
    def _():
        tile = step - n_heads_steps
        full = jnp.dot(heads_out[...], out_block(), preferred_element_type=jnp.float32).astype(jnp.bfloat16)
        part[2 * tile] = full[:seq]
        part[2 * tile + 1] = full[seq:2 * seq]

        @pl.when(tile < kept)
        def _():
            partb[tile] = full[2 * seq:]
            to_partner(tile).start()

        @pl.when(tile >= kept)
        def _():
            part[n_line1 + tile - kept] = full[2 * seq:]

        @pl.when(is_end)
        def _():
            end_to_inner(2 * tile).start()
            end_to_inner(2 * tile + 1).start()

            @pl.when(tile >= kept)
            def _():
                end_to_inner(n_line1 + tile - kept).start()

    @pl.when(is_relay & in_tiles)
    def _():
        c = 2 * (step - n_heads_steps) + 1
        part[c] = jnp.dot(heads_out[:seq], out_block(), preferred_element_type=jnp.float32).astype(jnp.bfloat16)

        @pl.when(is_end)
        def _():
            end_to_inner(c).start()

    def tick(tau):
        own = tau - jnp.where(is_relay, HOP_LAG, 0)
        arrives = is_relay & (lax.rem(own + 2 * n_chunks, 2) == 0)

        @pl.when(arrives & on_line(own))
        def _():
            to_partner(lax.div(own, 2)).wait_recv()

            @pl.when(is_end)
            def _():
                end_to_inner(own).start()

        first = own - HOP_LAG

        @pl.when(is_inner & on_line(first))
        def _():
            end_to_inner(first).wait_recv()

            part[first] = (part[first].astype(jnp.float32) + ebuf[first].astype(jnp.float32)).astype(jnp.bfloat16)
            inner_to_peer(first).start()

        second = first - HOP_LAG

        @pl.when(is_inner & on_line(second))
        def _():
            inner_to_peer(second).wait_recv()
            ebuf[second] = (part[second].astype(jnp.float32) + ibuf[second].astype(jnp.float32)).astype(jnp.bfloat16)
            final_to_end(second).start()
            deliver(second, ebuf)

        third = second - HOP_LAG

        @pl.when(is_end & on_line(third))
        def _():
            final_to_end(third).wait_recv()
            deliver(third, ibuf)

    n_ticks = max(n_chunks + 3 * HOP_LAG, n_line1 + 4 * HOP_LAG)

    def ticks_done(at):
        tile = at - n_heads_steps
        return jnp.where(tile < 0, 0, jnp.where(tile < n_tiles, 2 * (tile + 1), n_ticks))

    @pl.loop(ticks_done(step - 1), ticks_done(step))
    def _(tau):
        tick(tau)

    @pl.when(drain)
    def _():
        @pl.loop(0, n_chunks)
        def _(c):
            @pl.when(is_end & on_line(c))
            def _():
                end_to_inner(c).wait_send()

            @pl.when(is_inner & on_line(c))
            def _():
                inner_to_peer(c).wait_send()
                final_to_end(c).wait_send()

            @pl.when(is_prompt)
            def _():
                final_local(c, part).wait()

            @pl.when(is_prompt & on_relay_line(c))
            def _():
                final_back(c, part).wait_recv()

            @pl.when(is_relay & on_line(c))
            def _():
                final_back(c, part).wait_send()

        @pl.when(is_prompt)
        def _():
            @pl.when(t < 3)
            def _():
                cache_copy().wait_send()

            @pl.loop(0, kept)
            def _(tile):
                to_partner(tile).wait_send()

            @pl.loop(0, n_pieces)
            def _(p):
                tokens_over(p).wait_send()

        @pl.when(is_relay)
        def _():
            @pl.when(t < 3)
            def _():
                cache_copy().wait_recv()

            @pl.when(t == 3)
            def _():
                cache_own().wait()

            @pl.loop(0, n_pieces)
            def _(p):
                tokens_next(p, side).wait_send()


def prefill(tokens, w_query, w_dkv, gain, w_uk, w_uv, w_out, seq_len):
    rows, width = tokens.shape
    depth = w_out.shape[0]
    kv_rank = w_uk.shape[0]
    n_heads_steps = depth // (HEADS_STEP * V_DIM)
    n_tiles = width // TILE
    prompt_rows = rows - seq_len
    latent_width = w_dkv.shape[0]
    n_pieces = seq_len // 2 // PIECE

    def head_block(i):
        return jnp.minimum(i, n_heads_steps - 1)

    any_spec = pl.BlockSpec(memory_space=pl.ANY)
    tabs = lane_tables(seq_len)
    tab_spec = pl.BlockSpec((seq_len, 128), lambda i: (0, 0))
    chunk = pltpu.VMEM((2 * n_tiles + SHIFTED, seq_len, TILE), jnp.bfloat16)
    sems = [n_pieces] * 4 + [n_tiles] * 2 + [2 * n_tiles + SHIFTED] * 8 + [2, 2, 2]
    return pl.pallas_call(
        functools.partial(prefill_kernel, n_heads_steps, n_tiles),
        grid=(n_heads_steps + n_tiles + 1,),
        out_shape=(jax.ShapeDtypeStruct((rows, width), jnp.bfloat16), jax.ShapeDtypeStruct((seq_len, latent_width), jnp.bfloat16)),
        in_specs=[
            any_spec,
            any_spec,
            pl.BlockSpec((kv_rank, HEADS_STEP * NOPE_DIM), lambda i: (0, head_block(i))),
            pl.BlockSpec((kv_rank, HEADS_STEP * V_DIM), lambda i: (0, head_block(i))),
            pl.BlockSpec((kv_rank,), lambda i: (0,)),
            tab_spec, tab_spec, tab_spec, tab_spec,
            any_spec,
            any_spec,
        ],
        out_specs=(any_spec, any_spec),
        scratch_shapes=[
            pltpu.VMEM((prompt_rows, width), jnp.bfloat16),
            pltpu.VMEM((2, width, HEADS_STEP * (NOPE_DIM + ROPE_DIM)), jnp.bfloat16),
            pltpu.VMEM((latent_width, width), jnp.bfloat16),
            pltpu.VMEM((prompt_rows, kv_rank + 128), jnp.bfloat16),
            pltpu.VMEM((prompt_rows, latent_width), jnp.bfloat16),
            pltpu.VMEM((2, prompt_rows, HEADS_STEP * (NOPE_DIM + ROPE_DIM)), jnp.bfloat16),
            pltpu.VMEM((2, prompt_rows, HEADS_STEP * NOPE_DIM), jnp.bfloat16),
            pltpu.VMEM((2, prompt_rows, HEADS_STEP * V_DIM), jnp.bfloat16),
            pltpu.VMEM((prompt_rows, depth), jnp.bfloat16),
            chunk,
            pltpu.VMEM((n_tiles, seq_len, TILE), jnp.bfloat16),
            chunk,
            chunk,
        ] + [pltpu.SemaphoreType.DMA((n,)) for n in sems],
        compiler_params=pltpu.CompilerParams(collective_id=0, has_side_effects=True, vmem_limit_bytes=67043328),
    )(tokens, w_query, w_uk, w_uv, gain, *tabs, w_out, w_dkv)


def solution(mesh):
    half_stage = mesh.shape["stage"] // 2
    slot_spec = P(("dp", "stage"), None, None, None)
    cache_spec = P(("dp", "stage"), "t", None, None)

    def device_step(hidden, w_query, w_dkv, latent_gain, w_uk, w_uv, w_out):
        batch, seq_len, width = hidden.shape[1:]
        summed, handed = prefill(hidden.reshape(batch * seq_len, width), w_query, w_dkv.T, latent_gain, w_uk, w_uv, w_out, seq_len)
        is_prompt = lax.axis_index("stage") < half_stage
        out_rows = jnp.where(is_prompt, summed, jnp.zeros_like(summed)).reshape(1, batch, seq_len, width)
        cache = jnp.where(is_prompt, jnp.zeros_like(handed), handed)
        return out_rows, cache[None, None]

    return jax.shard_map(device_step, mesh=mesh, in_specs=(slot_spec, P(None, "t"), P(None, None), P(None), P(None, "t"), P(None, "t"), P("t", None)), out_specs=(slot_spec, cache_spec), check_vma=False)
```
